512 devices in a mesh: row: 64 (over z_lo, y, core), vec: 8 (over z_hi, x).
Axes of the slice: x: 4, y: 8, z: 8 (z_hi: 2, z_lo: 4; z = z_hi * 4 + z_lo), core: 2. Of those that a mesh axis runs over, the one named last changes fastest.
Arguments:
- eigvecs: float32 [32768, 8192], P('row', 'vec'), may hold values from -6 to 6
- reflectors: float32 [6, 32768, 128], P(None, 'row', 'vec'), may hold values from -0.375 to 0.375
- factors: float32 [6, 128, 128, 128], P(None, 'row', 'vec'), may hold values from -0.25 to 0.25
Outputs:
- vectors: float32 [32768, 8192], P('row', 'vec')
The draws below stay inside these ranges and needn't reach their ends.
All inputs are finite; a program needn't handle non-finite values.
Results may differ from the reference program's by a relative error of at most 0.0001.
Values sent between devices are 32-bit elements; how exact they have to be, the bound alone decides.
No kernel may reach another device: no remote copies, remote signals or barrier semaphores. Data moves between devices by JAX's collectives and lax.ppermute only.
A program may use at most 64 MiB of HBM per device.

```python
import jax
import jax.numpy as jnp
from jax import lax

NB = 128
ROUNDS = 6
ROWS = 32768
COLS = 8192
GROUPS = 128


def steps_of(rng, shape, pieces, smallest, high):
    factor_of = 1.0
    for position, shards_of in pieces:
        heights = jax.random.uniform(jax.random.fold_in(jax.random.fold_in(rng, 6), position), (shards_of,), jnp.float32, smallest / len(pieces), high / len(pieces))
        factor_of = factor_of * jnp.repeat(jnp.exp(heights), shape[position] // shards_of).reshape((-1,) + (1,) * (len(shape) - 1 - position))
    return factor_of


def noise(own_key, shape, deviation, bound, cuts=(), held_as=jnp.bfloat16):
    array = deviation * jax.random.normal(own_key, shape, jnp.float32)
    if cuts:
        array = array * steps_of(own_key, shape, cuts, -0.22, 0.18)
    return jnp.clip(array, -bound, bound).astype(held_as)


def setup_inputs(seed: int = 0) -> dict:
    key_list = jax.random.split(jax.random.key(seed), 4)
    return {
        "eigvecs": noise(key_list[0], (ROWS, COLS), 1.0, 6.0, ((0, 64), (1, 8)), jnp.float32),
        "reflectors": noise(key_list[1], (ROUNDS, ROWS, NB), (2 * NB) ** -0.5, 0.375, ((1, 64), (2, 8)), jnp.float32),
        "factors": noise(key_list[2], (ROUNDS, GROUPS, NB, NB), (4 * NB) ** -0.5, 0.25, ((1, 64), (2, 8)), jnp.float32),
    }


highest = lax.Precision.HIGHEST


def apply_groups(panel, basis, blocks):
    inner = jnp.einsum('gri,grc->gic', basis, panel, precision=highest)
    images = jnp.einsum('gij,gjc->gic', blocks, inner, precision=highest)
    return panel - jnp.einsum('gri,gic->grc', basis, images, precision=highest)


def reference(eigvecs, reflectors, factors):
    vectors = eigvecs
    total = vectors.shape[0]
    width = vectors.shape[1]
    for number in range(ROUNDS):
        offset = number * NB
        count = (total - offset + 2 * NB - 1) // (2 * NB)
        filler = count * 2 * NB - (total - offset)
        panel = jnp.pad(vectors[offset:], ((0, filler), (0, 0))).reshape(count, 2 * NB, width)
        basis = jnp.pad(reflectors[number, offset:], ((0, filler), (0, 0))).reshape(count, 2 * NB, NB)
        panel = apply_groups(panel, basis, factors[number, :count])
        vectors = jnp.concatenate([vectors[:offset], panel.reshape(count * 2 * NB, width)[:total - offset]], 0)
    return vectors
```

```python
import jax
import jax.numpy as jnp
from jax import lax
from jax.experimental import pallas as pl
from jax.experimental.pallas import tpu as pltpu
from jax.sharding import PartitionSpec as P

NB = 128
F32 = jnp.float32
BF16 = jnp.bfloat16
SPAN = 512
XS = 4


def split(x):
    high = x.astype(BF16)
    return high, (x - high.astype(F32)).astype(BF16)


def mm(a, b):
    return jnp.dot(a, b, preferred_element_type=F32)


def dot3(a, b):
    return mm(a[0], b[0]) + (mm(a[0], b[1]) + mm(a[1], b[0]))


def product(a, b):
    return dot3(split(a), split(b))


def assemble(buf, where, start, stop):
    here = where[0]
    rows = [
        buf[x, pl.ds(pl.multiple_of((here if z == 0 else 1 - here) * 16, 16), 16), start:stop]
        for z in range(2)
        for x in range(XS)
    ]
    return jnp.concatenate(rows, axis=0)


def group_matrix(basis_t, block):
    return product(basis_t.T, product(block, basis_t))


def put(refs, index, value):
    high, low = split(value)
    refs[0][index] = high
    refs[1][index] = low


def get(refs, *index):
    return refs[0][index], refs[1][index]


def look_ahead(side, nxt_t, matrix):
    zero = jnp.zeros((NB, NB), F32)
    if side == 0:
        return jnp.concatenate([nxt_t, zero], axis=1) - product(nxt_t, matrix[:NB])
    return jnp.concatenate([zero, nxt_t], axis=1) - product(nxt_t, matrix[NB:])


def spans(body, width):
    def step(c, carry):
        body(pl.ds(pl.multiple_of(c * SPAN, SPAN), SPAN))
        return carry

    lax.fori_loop(0, width // SPAN, step, 0)


def first_kernel(where, buf, x, u, chip, core, oph, opl):
    op = (oph, opl)
    basis = assemble(buf, where, 0, 512)
    for side in range(2):
        nxt = assemble(buf, where, 512 + side * NB, 512 + (side + 1) * NB)
        block = assemble(buf, where, 768 + side * NB, 768 + (side + 1) * NB)
        matrix = group_matrix(basis[:, side * 256 : side * 256 + 256], block)
        put(op, side, jnp.concatenate([matrix, look_ahead(side, nxt, matrix)], axis=0))
    odd = where[1] == 1

    def body(cols):
        heads = []
        for side in range(2):
            rows = slice(side * 256, side * 256 + 256)
            panel = x[rows, cols]
            image = dot3(get(op, side), split(panel))
            u[rows, cols] = panel - image[:256]
            heads.append(image[256:])
        chip[:, cols] = jnp.where(odd, heads[1], heads[0])
        core[:, cols] = jnp.where(odd, heads[0], heads[1])

    spans(body, x.shape[1])


def middle_kernel(prev_at, last, where, prev, buf, u_in, *rest):
    if last:
        u, uh, ul, mh, ml = rest
    else:
        u, ph, pl_, uh, ul, qh, ql, ahead, mh, ml, lh, ll = rest
    mid = (mh, ml)
    put(mid, slice(None), group_matrix(assemble(buf, where, 0, 256), assemble(buf, where, 256, 384)))
    spread = []
    for side in range(2):
        basis = assemble(prev, where, prev_at + side * NB, prev_at + (side + 1) * NB)
        at = 512 if side == 0 else 384
        value = product(basis.T, assemble(buf, where, at, at + NB))
        put((uh, ul), side, value)
        spread.append(value)
    if not last:
        basis = assemble(buf, where, 640, 1152)
        for side in range(2):
            block = assemble(buf, where, 1152 + side * NB, 1152 + (side + 1) * NB)
            nxt = assemble(buf, where, 1408 + side * NB, 1408 + (side + 1) * NB)
            matrix = group_matrix(basis[:, side * 256 : side * 256 + 256], block)
            put((ph, pl_), side, matrix)
            look = look_ahead(side, nxt, matrix)
            put((lh, ll), side, look)
            put((qh, ql), side, product(look[:, :NB] if side == 0 else look[:, NB:], spread[side]))

    def body(cols):
        panel = u_in[128:384, cols]
        panel = panel - dot3(get(mid, slice(None)), split(panel))
        u[128:384, cols] = panel
        top, bottom = u_in[0:128, cols], u_in[384:512, cols]
        u[0:128, cols] = top
        u[384:512, cols] = bottom
        if not last:
            ahead[0, :, cols] = dot3(get((lh, ll), 0), split(jnp.concatenate([top, panel[:NB]], axis=0)))
            ahead[1, :, cols] = dot3(get((lh, ll), 1), split(jnp.concatenate([panel[NB:], bottom], axis=0)))

    spans(body, u.shape[1])


def next_kernel(where, own_chip, got_chip, own_core, got_core, qh, ql, ahead, chip, core):
    odd = where[1]

    def body(cols):
        for own, got, out, side in ((own_chip, got_chip, chip, odd), (own_core, got_core, core, 1 - odd)):
            total = own[:, cols] + got[:, cols]
            out[:, cols] = ahead[side, :, cols] - dot3((qh[side], ql[side]), split(total))

    spans(body, chip.shape[1])


def even_kernel(last, where, own_chip, got_chip, own_core, got_core, uh, ul, *rest):
    if last:
        u_in, u = rest
    else:
        ph, pl_, u_in, u = rest
    odd = where[1] == 1

    def body(cols):
        chip = own_chip[:, cols] + got_chip[:, cols]
        core = own_core[:, cols] + got_core[:, cols]
        totals = (jnp.where(odd, core, chip), jnp.where(odd, chip, core))
        for side in range(2):
            near = slice(0, 128) if side == 0 else slice(384, 512)
            far = slice(128, 256) if side == 0 else slice(256, 384)
            panel = u_in[near, cols] - dot3((uh[side], ul[side]), split(totals[side]))
            if last:
                u[near, cols] = panel
                u[far, cols] = u_in[far, cols]
            else:
                rows = slice(side * 256, side * 256 + 256)
                pair = [panel, u_in[far, cols]] if side == 0 else [u_in[far, cols], panel]
                both = jnp.concatenate(pair, axis=0)
                u[rows, cols] = both - dot3((ph[side], pl_[side]), split(both))

    spans(body, u.shape[1])


def call(kernel, name, outs, scratch, flops, *args):
    smem = pl.BlockSpec(memory_space=pltpu.SMEM)
    vmem = pl.BlockSpec(memory_space=pltpu.VMEM)
    return pl.pallas_call(
        kernel,
        name=name,
        out_shape=[jax.ShapeDtypeStruct(s, t) for s, t in outs],
        in_specs=[smem] + [vmem] * (len(args) - 1),
        out_specs=[vmem] * len(outs),
        scratch_shapes=[pltpu.VMEM(s, t) for s, t in scratch],
        cost_estimate=pl.CostEstimate(flops=flops, bytes_accessed=4 << 20, transcendentals=0),
        compiler_params=pltpu.CompilerParams(vmem_limit_bytes=24 << 20),
    )(*args)


def gather(payload, far_pairs, near_groups):
    other = lax.ppermute(payload, "vec", far_pairs)
    both = jnp.concatenate([payload, other], axis=0)
    spread = jnp.broadcast_to(both, (XS, *both.shape))
    return lax.all_to_all(spread, "vec", 0, 0, tiled=True, axis_index_groups=near_groups)


def per_device(eigvecs, reflectors, factors):
    vec = lax.axis_index("vec")
    row = lax.axis_index("row")
    rows = lax.axis_size("row")
    where = jnp.stack([vec // XS, row % 2]).astype(jnp.int32)
    far_pairs = [(v, (v + XS) % (2 * XS)) for v in range(2 * XS)]
    near_groups = [list(range(XS)), list(range(XS, 2 * XS))]
    chip_pairs = [p for k in range(1, rows - 1, 2) for p in ((k, k + 1), (k + 1, k))]
    core_pairs = [(k, k ^ 1) for k in range(rows)]

    turned = jnp.transpose(reflectors, (0, 2, 1))
    slid = lax.ppermute(
        jnp.concatenate(
            [factors[r, g] for r, g in ((1, 1), (2, 1), (3, 0), (3, 1), (4, 0), (4, 1), (5, 0), (5, 1))], axis=1
        ),
        "row",
        [(k, k + 1) for k in range(rows - 1)],
    )
    s = [slid[:, k * NB : (k + 1) * NB] for k in range(8)]
    slid2 = lax.ppermute(factors[5, 1], "row", [(k, k + 2) for k in range(rows - 2)])

    def ends(r):
        return [turned[r, :, :NB], turned[r, :, 3 * NB :]]

    def joined(parts):
        return jnp.concatenate(parts, axis=1)

    a = joined([turned[0], *ends(1), factors[0, 0], factors[0, 1]])
    b = joined([turned[1, :, NB : 3 * NB], factors[1, 0], factors[1, 1], s[0], turned[2], s[1], factors[2, 0], *ends(3)])
    c = joined([turned[3, :, NB : 3 * NB], s[3], factors[3, 0], s[2], turned[4], s[4], s[5], *ends(5)])
    d = joined([turned[5, :, NB : 3 * NB], s[6], s[7], slid2])
    a, b, c, d = (gather(part, far_pairs, near_groups) for part in (a, b, c, d))

    width = eigvecs.shape[1]
    whole = ((4 * NB, width), F32)
    strip = ((NB, width), F32)
    pair = ((2, 2 * NB, 2 * NB), BF16)
    small = ((2, NB, NB), BF16)
    strips = ((2, NB, width), F32)
    look = ((2, NB, 2 * NB), BF16)
    mid = ((2 * NB, 2 * NB), BF16)
    op = ((2, 3 * NB, 2 * NB), BF16)

    def swap(chip, core):
        return lax.ppermute(chip, "row", chip_pairs), lax.ppermute(core, "row", core_pairs)

    unit = 2 * NB * NB * width * 3
    u, chip, core = call(first_kernel, "first", [whole, strip, strip], [op, op], 12 * unit, where, a, eigvecs)
    prev, prev_at = a, 512
    for buf in (b, c):
        got_chip, got_core = swap(chip, core)
        u, ph, pl_, uh, ul, qh, ql, ahead = call(
            lambda *refs, at=prev_at: middle_kernel(at, False, *refs),
            "middle",
            [whole, pair, pair, small, small, small, small, strips],
            [mid, mid, look, look],
            10 * unit,
            where, prev, buf, u,
        )
        new_chip, new_core = call(
            next_kernel, "next", [strip, strip], [], 2 * unit, where, chip, got_chip, core, got_core, qh, ql, ahead
        )
        (u,) = call(
            lambda *refs: even_kernel(False, *refs),
            "even",
            [whole],
            [],
            10 * unit,
            where, chip, got_chip, core, got_core, uh, ul, ph, pl_, u,
        )
        chip, core = new_chip, new_core
        prev, prev_at = buf, 1408
    got_chip, got_core = swap(chip, core)
    u, uh, ul = call(
        lambda *refs: middle_kernel(prev_at, True, *refs),
        "middle_last",
        [whole, small, small],
        [mid, mid],
        5 * unit,
        where, prev, d, u,
    )
    (u,) = call(
        lambda *refs: even_kernel(True, *refs),
        "last",
        [whole],
        [],
        2 * unit,
        where, chip, got_chip, core, got_core, uh, ul, u,
    )
    return u


def solution(mesh):
    return jax.shard_map(
        per_device,
        mesh=mesh,
        in_specs=(P("row", "vec"), P(None, "row", "vec"), P(None, "row", "vec", None)),
        out_specs=P("row", "vec"),
        check_vma=False,
    )
```

```python
import jax
import jax.numpy as jnp
from jax import lax
from jax.experimental import pallas as pl
from jax.experimental.pallas import tpu as pltpu
from jax.sharding import PartitionSpec as P


NB = 128
F32 = jnp.float32
BF16 = jnp.bfloat16
SPAN = 512
XS = 4
SHIFTED = ((1, 1), (2, 1), (3, 0), (3, 1), (4, 0), (4, 1), (5, 0), (5, 1))


def split(x):
    high = x.astype(BF16)
    return high, (x - high.astype(F32)).astype(BF16)


def mm(a, b):
    return jnp.dot(a, b, preferred_element_type=F32)


def dot3(a, b):
    return mm(a[0], b[0]) + (mm(a[0], b[1]) + mm(a[1], b[0]))


def product(a, b):
    return dot3(split(a), split(b))


def place():
    vec = lax.axis_index("vec")
    return lax.shift_right_logical(vec, 2), vec & 3, lax.axis_index("row") & 1


def assemble(parts, buf, start=0):
    far, near, _ = place()
    width = buf.shape[2]
    for step, part in zip((0, -1, 1, 2), parts):
        x = (near + step) & 3
        for z in range(2):
            buf[(far ^ z) * XS + x] = part[16 * z : 16 * z + 16, start : start + width]


def block(buf, start, width):
    return buf[:, :, start : start + width].reshape(NB, width)


def group_matrix(basis_t, factor):
    return product(basis_t.T, product(factor, basis_t))


def put(refs, index, value):
    high, low = split(value)
    refs[0][index] = high
    refs[1][index] = low


def get(refs, *index):
    return refs[0][index], refs[1][index]


def look_ahead(side, nxt_t, matrix):
    zero = jnp.zeros((NB, NB), F32)
    if side == 0:
        return jnp.concatenate([nxt_t, zero], axis=1) - product(nxt_t, matrix[:NB])
    return jnp.concatenate([zero, nxt_t], axis=1) - product(nxt_t, matrix[NB:])


def spans(body, width):
    def step(c, carry):
        body(pl.ds(pl.multiple_of(c * SPAN, SPAN), SPAN))
        return carry

    lax.fori_loop(0, width // SPAN, step, 0)


def first_payload_kernel(turned, factors, out, shifted, turned_here, factors_here, sem):
    copies = [
        pltpu.make_async_copy(turned, turned_here, sem.at[0]),
        pltpu.make_async_copy(factors, factors_here, sem.at[1]),
    ]
    for copy in copies:
        copy.start()
    for copy in copies:
        copy.wait()
    out[:, 0:512] = turned_here[0]
    out[:, 512:640] = turned_here[1, :, 0:128]
    out[:, 640:768] = turned_here[1, :, 384:512]
    out[:, 768:896] = factors_here[0, 0]
    out[:, 896:1024] = factors_here[0, 1]
    for k, (r, g) in enumerate(SHIFTED):
        shifted[:, k * NB : (k + 1) * NB] = factors_here[r, g]


def rest_payload_kernel(turned, factors, slid, out):
    def came(k):
        return slid[:, k * NB : (k + 1) * NB]

    def middle(r):
        return turned[r, :, 128:384]

    def ends(r):
        return [turned[r, :, 0:128], turned[r, :, 384:512]]

    at = 0
    for part in (
        middle(1), factors[1, 0], factors[1, 1], came(0), turned[2], came(1), factors[2, 0], *ends(3),
        middle(3), came(3), factors[3, 0], came(2), turned[4], came(4), came(5), *ends(5),
        middle(5), came(6), came(7),
    ):
        out[:, at : at + part.shape[1]] = part
        at += part.shape[1]


def first_kernel(own, left, right, across, x, u, chip, core, nxt_t, buf, oph, opl):
    op = (oph, opl)
    assemble((own, left, right, across), buf)
    odd = place()[2] == 1
    for side in range(2):
        nxt = block(buf, 512 + side * NB, NB)
        nxt_t[side] = nxt
        matrix = group_matrix(block(buf, side * 256, 256), block(buf, 768 + side * NB, NB))
        put(op, side, jnp.concatenate([matrix, look_ahead(side, nxt, matrix)], axis=0))

    def body(cols):
        heads = []
        for side in range(2):
            rows = slice(side * 256, side * 256 + 256)
            panel = x[rows, cols]
            image = dot3(get(op, side), split(panel))
            u[rows, cols] = panel - image[:256]
            heads.append(image[256:])
        chip[:, cols] = jnp.where(odd, heads[1], heads[0])
        core[:, cols] = jnp.where(odd, heads[0], heads[1])

    spans(body, x.shape[1])


def middle_kernel(number, own, left, right, across, prev_t, u_in, *rest):
    last = number == 3
    if number == 1:
        u, ph, pl_, uh, ul, qh, ql, ahead, nxt_t, extra, buf, mh, ml, lh, ll, tail = rest
        assemble((own, left, right, across), tail, 3 * 1280 - NB)
        for k in range(8):
            extra[:, k * NB : (k + 1) * NB] = tail[k]
    elif number == 2:
        u, ph, pl_, uh, ul, qh, ql, ahead, nxt_t, buf, mh, ml, lh, ll = rest
    else:
        got_chip, got_core, u, uh, ul, buf, mh, ml = rest
    mid = (mh, ml)
    assemble((own, left, right, across), buf, (number - 1) * 1664)
    at = 0
    put(mid, slice(None), group_matrix(block(buf, at, 256), block(buf, at + 256, NB)))
    spread = []
    for side in range(2):
        if last and side == 0:
            came = jnp.where(place()[2] == 1, got_core[NB:, :], got_chip[NB:, :])
            factor = jnp.concatenate([came[:, k * NB : (k + 1) * NB] for k in range(8)], axis=0)
        else:
            factor = block(buf, at + (512 if side == 0 else 384), NB)
        value = product(prev_t[side].T, factor)
        put((uh, ul), side, value)
        spread.append(value)
    if not last:
        for side in range(2):
            factor = block(buf, at + 1152 + side * NB, NB)
            nxt = block(buf, at + 1408 + side * NB, NB)
            nxt_t[side] = nxt
            matrix = group_matrix(block(buf, at + 640 + side * 256, 256), factor)
            put((ph, pl_), side, matrix)
            look = look_ahead(side, nxt, matrix)
            put((lh, ll), side, look)
            put((qh, ql), side, product(look[:, :NB] if side == 0 else look[:, NB:], spread[side]))

    def body(cols):
        panel = u_in[128:384, cols]
        panel = panel - dot3(get(mid, slice(None)), split(panel))
        u[128:384, cols] = panel
        top, bottom = u_in[0:128, cols], u_in[384:512, cols]
        u[0:128, cols] = top
        u[384:512, cols] = bottom
        if not last:
            ahead[0, :, cols] = dot3(get((lh, ll), 0), split(jnp.concatenate([top, panel[:NB]], axis=0)))
            ahead[1, :, cols] = dot3(get((lh, ll), 1), split(jnp.concatenate([panel[NB:], bottom], axis=0)))

    spans(body, u.shape[1])


def next_kernel(own_chip, got_chip, own_core, got_core, qh, ql, ahead, *rest):
    *extra, chip, core = rest
    odd = place()[2]
    for value in extra:
        chip[NB:, :] = value[...]
        core[NB:, :] = value[...]

    def body(cols):
        for own, got, out, side in ((own_chip, got_chip, chip, odd), (own_core, got_core, core, 1 - odd)):
            total = own[:NB, cols] + got[:NB, cols]
            out[:NB, cols] = ahead[side, :, cols] - dot3((qh[side], ql[side]), split(total))

    spans(body, chip.shape[1])


def even_kernel(last, own_chip, got_chip, own_core, got_core, uh, ul, *rest):
    if last:
        u_in, u = rest
    else:
        ph, pl_, u_in, u = rest
    odd = place()[2] == 1

    def body(cols):
        chip = own_chip[:NB, cols] + got_chip[:NB, cols]
        core = own_core[:NB, cols] + got_core[:NB, cols]
        totals = (jnp.where(odd, core, chip), jnp.where(odd, chip, core))
        for side in range(2):
            near = slice(0, 128) if side == 0 else slice(384, 512)
            far = slice(128, 256) if side == 0 else slice(256, 384)
            panel = u_in[near, cols] - dot3((uh[side], ul[side]), split(totals[side]))
            if last:
                u[near, cols] = panel
                u[far, cols] = u_in[far, cols]
            else:
                rows = slice(side * 256, side * 256 + 256)
                pair = [panel, u_in[far, cols]] if side == 0 else [u_in[far, cols], panel]
                both = jnp.concatenate(pair, axis=0)
                u[rows, cols] = both - dot3((ph[side], pl_[side]), split(both))

    spans(body, u.shape[1])


def call(kernel, outs, scratch, flops, *args, far=(), sems=0):
    vmem = pl.BlockSpec(memory_space=pltpu.VMEM)
    hbm = pl.BlockSpec(memory_space=pltpu.HBM)
    return pl.pallas_call(
        kernel,
        out_shape=[jax.ShapeDtypeStruct(s, t) for s, t in outs],
        in_specs=[hbm if k in far else vmem for k in range(len(args))],
        out_specs=[vmem] * len(outs),
        scratch_shapes=[pltpu.VMEM(s, t) for s, t in scratch] + [pltpu.SemaphoreType.DMA((sems,))] * bool(sems),
        cost_estimate=pl.CostEstimate(flops=flops, bytes_accessed=4 << 20, transcendentals=0),
        compiler_params=pltpu.CompilerParams(vmem_limit_bytes=24 << 20),
    )(*args)


def far_half(payload):
    return lax.ppermute(payload, "vec", [(v, v ^ XS) for v in range(2 * XS)])


def near_parts(payload, other):
    both = jnp.concatenate([payload, other], axis=0)
    parts = [
        lax.ppermute(both, "vec", [(v, (v & XS) + ((v + step) & 3)) for v in range(2 * XS)])
        for step in (1, -1, 2)
    ]
    return (both, *parts)


def rounds(eigvecs, reflectors, factors):
    rows = lax.axis_size("row")
    chip_pairs = [p for k in range(1, rows - 1, 2) for p in ((k, k + 1), (k + 1, k))]
    core_pairs = [(k, k ^ 1) for k in range(rows)]
    turned = jnp.transpose(reflectors, (0, 2, 1))
    a, shifted, turned, factors = call(
        first_payload_kernel,
        [((16, 1024), F32), ((16, 1024), F32), (turned.shape, F32), (factors.shape, F32)],
        [],
        1 << 20,
        turned,
        factors,
        far=(0, 1),
        sems=2,
    )
    slid = lax.ppermute(shifted, "row", [(k, k + 1) for k in range(rows - 1)])
    a2 = far_half(a)
    (b,) = call(rest_payload_kernel, [((16, 3840), F32)], [], 1 << 20, turned, factors, slid)
    b2 = far_half(b)
    a = near_parts(a, a2)
    b = near_parts(b, b2)

    width = eigvecs.shape[1]
    whole = ((4 * NB, width), F32)
    strip = ((NB, width), F32)
    pair = ((2, 2 * NB, 2 * NB), BF16)
    small = ((2, NB, NB), BF16)
    ends = ((2, NB, NB), F32)
    strips = ((2, NB, width), F32)
    look = ((2, NB, 2 * NB), BF16)
    mid = ((2 * NB, 2 * NB), BF16)
    op = ((2, 3 * NB, 2 * NB), BF16)

    def held(lanes):
        return ((2 * XS, 16, lanes), F32)

    def swap(chip, core):
        return lax.ppermute(chip, "row", chip_pairs), lax.ppermute(core, "row", core_pairs)

    unit = 2 * NB * NB * width * 3
    u, chip, core, nxt_t = call(first_kernel, [whole, strip, strip, ends], [held(1024), op, op], 12 * unit, *a, eigvecs)
    longer = ((NB + 16, width), F32)
    for number in (1, 2):
        got_chip, got_core = swap(chip, core)
        u, ph, pl_, uh, ul, qh, ql, ahead, nxt_t, *extra = call(
            lambda *refs, number=number: middle_kernel(number, *refs),
            [whole, pair, pair, small, small, small, small, strips, ends] + [((16, width), F32)] * (2 - number),
            [held(1664), mid, mid, look, look] + [held(NB)] * (2 - number),
            10 * unit,
            *b, nxt_t, u,
        )
        sent = longer if number == 1 else strip
        new_chip, new_core = call(
            next_kernel,
            [sent, sent],
            [],
            2 * unit,
            chip, got_chip, core, got_core, qh, ql, ahead, *extra,
        )
        (u,) = call(
            lambda *refs: even_kernel(False, *refs),
            [whole],
            [],
            10 * unit,
            chip, got_chip, core, got_core, uh, ul, ph, pl_, u,
        )
        if number == 2:
            came_chip, came_core = got_chip, got_core
        chip, core = new_chip, new_core
    got_chip, got_core = swap(chip, core)
    u, uh, ul = call(
        lambda *refs: middle_kernel(3, *refs),
        [whole, small, small],
        [held(512), mid, mid],
        5 * unit,
        *b, nxt_t, u, came_chip, came_core,
    )
    (u,) = call(
        lambda *refs: even_kernel(True, *refs),
        [whole],
        [],
        2 * unit,
        chip, got_chip, core, got_core, uh, ul, u,
    )
    return u


def solution(mesh):
    return jax.shard_map(
        rounds,
        mesh=mesh,
        in_specs=(P("row", "vec"), P(None, "row", "vec"), P(None, "row", "vec", None)),
        out_specs=P("row", "vec"),
        check_vma=False,
    )
```

```python
import jax
import jax.numpy as jnp
from jax import lax
from jax.experimental import pallas as pl
from jax.experimental.pallas import tpu as pltpu
from jax.sharding import PartitionSpec as P


NB = 128
F32 = jnp.float32
BF16 = jnp.bfloat16
SPAN = 512
XS = 4
SHIFTED = ((1, 1), (2, 1), (3, 0), (3, 1), (4, 0), (4, 1), (5, 0), (5, 1))


def split(x):
    high = x.astype(BF16)
    return high, (x - high.astype(F32)).astype(BF16)


def mm(a, b):
    return jnp.dot(a, b, preferred_element_type=F32)


def dot3(a, b):
    return mm(a[0], b[0]) + (mm(a[0], b[1]) + mm(a[1], b[0]))


def product(a, b):
    return dot3(split(a), split(b))


def place():
    vec = lax.axis_index("vec")
    return lax.shift_right_logical(vec, 2), vec & 3, lax.axis_index("row") & 1


def assemble(parts, buf, start=0):
    far, near, _ = place()
    width = buf.shape[2]
    for step, part in zip((0, 1, 3, 2), parts):
        x = near ^ step
        for z in range(2):
            buf[(far ^ z) * XS + x] = part[16 * z : 16 * z + 16, start : start + width]


def block(buf, start, width):
    return buf[:, :, start : start + width].reshape(NB, width)


def group_matrix(basis_t, factor):
    return product(basis_t.T, product(factor, basis_t))


def put(refs, index, value):
    high, low = split(value)
    refs[0][index] = high
    refs[1][index] = low


def get(refs, *index):
    return refs[0][index], refs[1][index]


def look_ahead(side, nxt_t, matrix):
    zero = jnp.zeros((NB, NB), F32)
    if side == 0:
        return jnp.concatenate([nxt_t, zero], axis=1) - product(nxt_t, matrix[:NB])
    return jnp.concatenate([zero, nxt_t], axis=1) - product(nxt_t, matrix[NB:])


def spans(body, width):
    def step(c, carry):
        body(pl.ds(pl.multiple_of(c * SPAN, SPAN), SPAN))
        return carry

    lax.fori_loop(0, width // SPAN, step, 0)


def first_payload_kernel(turned, factors, out, shifted, turned_here, factors_here, sem):
    copies = [
        pltpu.make_async_copy(turned, turned_here, sem.at[0]),
        pltpu.make_async_copy(factors, factors_here, sem.at[1]),
    ]
    for copy in copies:
        copy.start()
    for copy in copies:
        copy.wait()
    lay(
        out,
        turned_here[0], *ends(turned_here, 1), factors_here[0, 0], factors_here[0, 1],
        turned_here[1, :, 128:384], factors_here[1, 0], factors_here[1, 1],
    )
    lay(shifted, *(factors_here[r, g] for r, g in SHIFTED))


def lay(out, *parts):
    at = 0
    for part in parts:
        out[:, at : at + part.shape[1]] = part
        at += part.shape[1]


def ends(turned, r):
    return turned[r, :, 0:128], turned[r, :, 384:512]


def rest_payload_kernel(turned, factors, slid, out):
    came = [slid[:, k * NB : (k + 1) * NB] for k in range(8)]
    lay(
        out,
        came[0], turned[2], came[1], factors[2, 0], *ends(turned, 3),
        turned[3, :, 128:384], came[3], factors[3, 0], came[2], turned[4], came[4], came[5], *ends(turned, 5),
        turned[5, :, 128:384], came[6], came[7],
    )


def first_kernel(own, left, right, across, x, ph, pl_, chip, core, nxt_t, buf, lh, ll):
    assemble((own, left, right, across), buf)
    odd = place()[2] == 1
    for side in range(2):
        nxt = block(buf, 512 + side * NB, NB)
        nxt_t[side] = nxt
        matrix = group_matrix(block(buf, side * 256, 256), block(buf, 768 + side * NB, NB))
        put((ph, pl_), side, matrix)
        put((lh, ll), side, look_ahead(side, nxt, matrix))

    def body(cols):
        heads = [
            dot3(get((lh, ll), side), split(x[side * 256 : side * 256 + 256, cols])) for side in range(2)
        ]
        chip[:, cols] = jnp.where(odd, heads[1], heads[0])
        core[:, cols] = jnp.where(odd, heads[0], heads[1])

    spans(body, x.shape[1])


def fill_kernel(own, left, right, across, nxt_t, ph, pl_, x, u, tail, buf, mh, ml):
    assemble((own, left, right, across), buf, 1024)
    put((mh, ml), slice(None), group_matrix(block(buf, 0, 256), block(buf, 256, NB)))
    tail[...] = product(nxt_t[1].T, block(buf, 384, NB))

    def body(cols):
        panels = []
        for side in range(2):
            panel = x[side * 256 : side * 256 + 256, cols]
            panels.append(panel - dot3((ph[side], pl_[side]), split(panel)))
        u[0:128, cols] = panels[0][:NB]
        u[384:512, cols] = panels[1][NB:]
        panel = jnp.concatenate([panels[0][NB:], panels[1][:NB]], axis=0)
        u[128:384, cols] = panel - dot3((mh[...], ml[...]), split(panel))

    spans(body, u.shape[1])


def spread_and_ahead(buf, at, nxt_t, spread, ph, pl_, uh, ul, qh, ql, lh, ll):
    for side in range(2):
        put((uh, ul), side, spread[side])
        factor = block(buf, at + 512 + side * NB, NB)
        nxt = block(buf, at + 768 + side * NB, NB)
        nxt_t[side] = nxt
        matrix = group_matrix(block(buf, at + side * 256, 256), factor)
        put((ph, pl_), side, matrix)
        look = look_ahead(side, nxt, matrix)
        put((lh, ll), side, look)
        put((qh, ql), side, product(look[:, :NB] if side == 0 else look[:, NB:], spread[side]))


def ahead_kernel(own, left, right, across, prev_t, prev_tail, u, *rest):
    ph, pl_, uh, ul, qh, ql, ahead, nxt_t, extra, buf, last_block, lh, ll = rest
    assemble((own, left, right, across), last_block, 3328 - NB)
    for k in range(8):
        extra[:, k * NB : (k + 1) * NB] = last_block[k]
    assemble((own, left, right, across), buf)
    spread = (product(prev_t[0].T, block(buf, 0, NB)), prev_tail[...])
    spread_and_ahead(buf, NB, nxt_t, spread, ph, pl_, uh, ul, qh, ql, lh, ll)

    def body(cols):
        for side in range(2):
            rows = slice(side * 256, side * 256 + 256)
            ahead[side, :, cols] = dot3(get((lh, ll), side), split(u[rows, cols]))

    spans(body, u.shape[1])


def middle_kernel(own, left, right, across, prev_t, u_in, *rest):
    u, ph, pl_, uh, ul, qh, ql, ahead, nxt_t, buf, mh, ml, lh, ll = rest
    assemble((own, left, right, across), buf, 1152)
    put((mh, ml), slice(None), group_matrix(block(buf, 0, 256), block(buf, 256, NB)))
    spread = (product(prev_t[0].T, block(buf, 512, NB)), product(prev_t[1].T, block(buf, 384, NB)))
    spread_and_ahead(buf, 640, nxt_t, spread, ph, pl_, uh, ul, qh, ql, lh, ll)

    def body(cols):
        panel = u_in[128:384, cols]
        panel = panel - dot3((mh[...], ml[...]), split(panel))
        u[128:384, cols] = panel
        top, bottom = u_in[0:128, cols], u_in[384:512, cols]
        u[0:128, cols] = top
        u[384:512, cols] = bottom
        ahead[0, :, cols] = dot3(get((lh, ll), 0), split(jnp.concatenate([top, panel[:NB]], axis=0)))
        ahead[1, :, cols] = dot3(get((lh, ll), 1), split(jnp.concatenate([panel[NB:], bottom], axis=0)))

    spans(body, u.shape[1])


def final_middle_kernel(own, left, right, across, prev_t, u_in, got_chip, got_core, *rest):
    out, uh, ul, buf, mh, ml, rows, sem = rest
    assemble((own, left, right, across), buf, 2816)
    put((mh, ml), slice(None), group_matrix(block(buf, 0, 256), block(buf, 256, NB)))
    copies = []
    for c in range(u_in.shape[1] // SPAN):
        cols = slice(c * SPAN, c * SPAN + SPAN)
        panel = u_in[128:384, cols]
        rows[c] = panel - dot3((mh[...], ml[...]), split(panel))
        copies.append(pltpu.make_async_copy(rows.at[c], out.at[128:384, cols], sem.at[c]))
        copies[-1].start()
    came = jnp.where(place()[2] == 1, got_core[NB:, :], got_chip[NB:, :])
    head = jnp.concatenate([came[:, k * NB : (k + 1) * NB] for k in range(8)], axis=0)
    put((uh, ul), 0, product(prev_t[0].T, head))
    put((uh, ul), 1, product(prev_t[1].T, block(buf, 384, NB)))
    for copy in copies:
        copy.wait()


def next_kernel(own_chip, got_chip, own_core, got_core, qh, ql, ahead, *rest):
    *extra, chip, core = rest
    odd = place()[2]
    for value in extra:
        chip[NB:, :] = value[...]
        core[NB:, :] = value[...]

    def body(cols):
        for own, got, out, side in ((own_chip, got_chip, chip, odd), (own_core, got_core, core, 1 - odd)):
            total = own[:NB, cols] + got[:NB, cols]
            out[:NB, cols] = ahead[side, :, cols] - dot3((qh[side], ql[side]), split(total))

    spans(body, chip.shape[1])


def totals_of(own_chip, got_chip, own_core, got_core, cols):
    odd = place()[2] == 1
    chip = own_chip[:NB, cols] + got_chip[:NB, cols]
    core = own_core[:NB, cols] + got_core[:NB, cols]
    return jnp.where(odd, core, chip), jnp.where(odd, chip, core)


def even_kernel(own_chip, got_chip, own_core, got_core, uh, ul, ph, pl_, u_in, u):
    def body(cols):
        totals = totals_of(own_chip, got_chip, own_core, got_core, cols)
        for side in range(2):
            near = slice(0, 128) if side == 0 else slice(384, 512)
            far = slice(128, 256) if side == 0 else slice(256, 384)
            panel = u_in[near, cols] - dot3((uh[side], ul[side]), split(totals[side]))
            pair = [panel, u_in[far, cols]] if side == 0 else [u_in[far, cols], panel]
            both = jnp.concatenate(pair, axis=0)
            u[side * 256 : side * 256 + 256, cols] = both - dot3((ph[side], pl_[side]), split(both))

    spans(body, u.shape[1])


def last_kernel(own_chip, got_chip, own_core, got_core, uh, ul, u_in, held_out, out, rows, sem):
    del held_out
    copies = []
    for c in range(u_in.shape[1] // SPAN):
        cols = slice(c * SPAN, c * SPAN + SPAN)
        totals = totals_of(own_chip, got_chip, own_core, got_core, cols)
        for side in range(2):
            near = slice(0, 128) if side == 0 else slice(384, 512)
            k = 2 * c + side
            rows[k] = u_in[near, cols] - dot3((uh[side], ul[side]), split(totals[side]))
            copies.append(pltpu.make_async_copy(rows.at[k], out.at[near, cols], sem.at[k]))
            copies[-1].start()
    for copy in copies:
        copy.wait()


def call(kernel, outs, scratch, flops, *args, far=(), far_out=(), sems=0, aliases={}):
    vmem = pl.BlockSpec(memory_space=pltpu.VMEM)
    hbm = pl.BlockSpec(memory_space=pltpu.HBM)
    return pl.pallas_call(
        kernel,
        out_shape=[jax.ShapeDtypeStruct(s, t) for s, t in outs],
        in_specs=[hbm if k in far else vmem for k in range(len(args))],
        out_specs=[hbm if k in far_out else vmem for k in range(len(outs))],
        input_output_aliases=aliases,
        scratch_shapes=[pltpu.VMEM(s, t) for s, t in scratch] + [pltpu.SemaphoreType.DMA((sems,))] * bool(sems),
        cost_estimate=pl.CostEstimate(flops=flops, bytes_accessed=0 if far else 4 << 20, transcendentals=0),
        compiler_params=pltpu.CompilerParams(vmem_limit_bytes=24 << 20),
    )(*args)


def far_half(payload):
    return lax.ppermute(payload, "vec", [(v, v ^ XS) for v in range(2 * XS)])


def near_parts(payload, other):
    both = jnp.concatenate([payload, other], axis=0)
    parts = [lax.ppermute(both, "vec", [(v, v ^ step) for v in range(2 * XS)]) for step in (1, 3, 2)]
    return (both, *parts)


def rounds(eigvecs, reflectors, factors):
    rows = lax.axis_size("row")
    chip_pairs = [p for k in range(1, rows - 1, 2) for p in ((k, k + 1), (k + 1, k))]
    core_pairs = [(k, k ^ 1) for k in range(rows)]
    turned = jnp.transpose(reflectors, (0, 2, 1))
    a, shifted, turned, factors = call(
        first_payload_kernel,
        [((16, 1536), F32), ((16, 1024), F32), (turned.shape, F32), (factors.shape, F32)],
        [],
        1 << 20,
        turned,
        factors,
        far=(0, 1),
        sems=2,
    )
    slid = lax.ppermute(shifted, "row", [(k, k + 1) for k in range(rows - 1)])
    a2 = far_half(a)
    (b,) = call(rest_payload_kernel, [((16, 3328), F32)], [], 1 << 20, turned, factors, slid)
    b2 = far_half(b)
    a = near_parts(a, a2)
    b = near_parts(b, b2)

    width = eigvecs.shape[1]
    whole = ((4 * NB, width), F32)
    strip = ((NB, width), F32)
    pair = ((2, 2 * NB, 2 * NB), BF16)
    small = ((2, NB, NB), BF16)
    ends_t = ((2, NB, NB), F32)
    strips = ((2, NB, width), F32)
    look = ((2, NB, 2 * NB), BF16)
    mid = ((2 * NB, 2 * NB), BF16)

    def held(lanes):
        return ((2 * XS, 16, lanes), F32)

    def swap(chip, core):
        return lax.ppermute(chip, "row", chip_pairs), lax.ppermute(core, "row", core_pairs)

    unit = 2 * NB * NB * width * 3
    p0h, p0l, chip, core, nxt_t = call(
        first_kernel,
        [pair, pair, strip, strip, ends_t],
        [held(1024), look, look],
        4 * unit,
        *a, eigvecs,
    )
    got_chip, got_core = swap(chip, core)
    u, tail = call(
        fill_kernel,
        [whole, ((NB, NB), F32)],
        [held(512), mid, mid],
        12 * unit,
        *a, nxt_t, p0h, p0l, eigvecs,
    )
    ops = [pair, pair, small, small, small, small, strips, ends_t]
    ph, pl_, uh, ul, qh, ql, ahead, nxt_t, extra = call(
        ahead_kernel,
        [*ops, ((16, width), F32)],
        [held(1152), held(NB), look, look],
        4 * unit,
        *b, nxt_t, tail, u,
    )
    longer = ((NB + 16, width), F32)
    new_chip, new_core = call(
        next_kernel, [longer, longer], [], 2 * unit, chip, got_chip, core, got_core, qh, ql, ahead, extra
    )
    far_chip, far_core = swap(new_chip, new_core)
    (u,) = call(even_kernel, [whole], [], 10 * unit, chip, got_chip, core, got_core, uh, ul, ph, pl_, u)
    u, ph, pl_, uh, ul, qh, ql, ahead, nxt_t = call(
        middle_kernel,
        [whole, *ops],
        [held(1664), mid, mid, look, look],
        10 * unit,
        *b, nxt_t, u,
    )
    chip, core = new_chip, new_core
    new_chip, new_core = call(next_kernel, [strip, strip], [], 2 * unit, chip, far_chip, core, far_core, qh, ql, ahead)
    got_chip, got_core = swap(new_chip, new_core)
    (u,) = call(even_kernel, [whole], [], 10 * unit, chip, far_chip, core, far_core, uh, ul, ph, pl_, u)
    out, uh, ul = call(
        final_middle_kernel,
        [whole, small, small],
        [held(512), mid, mid, ((width // SPAN, 2 * NB, SPAN), F32)],
        5 * unit,
        *b, nxt_t, u, far_chip, far_core,
        far_out=(0,),
        sems=width // SPAN,
    )
    (out,) = call(
        last_kernel,
        [whole],
        [((2 * width // SPAN, NB, SPAN), F32)],
        2 * unit,
        new_chip, got_chip, new_core, got_core, uh, ul, u, out,
        far=(7,),
        far_out=(0,),
        sems=2 * width // SPAN,
        aliases={7: 0},
    )
    return out


def solution(mesh):
    return jax.shard_map(
        rounds,
        mesh=mesh,
        in_specs=(P("row", "vec"), P(None, "row", "vec"), P(None, "row", "vec", None)),
        out_specs=P("row", "vec"),
        check_vma=False,
    )
```

```python
import jax
import jax.numpy as jnp
from jax import lax
from jax.experimental import pallas as pl
from jax.experimental.pallas import tpu as pltpu
from jax.sharding import PartitionSpec as P


NB = 128
F32 = jnp.float32
BF16 = jnp.bfloat16
SPAN = 512
XS = 4
SHIFTED = ((1, 1), (2, 1), (3, 0), (3, 1), (4, 0), (4, 1), (5, 0), (5, 1))


def split(x):
    high = x.astype(BF16)
    return high, (x - high.astype(F32)).astype(BF16)


def mm(a, b):
    return jnp.dot(a, b, preferred_element_type=F32)


def dot3(a, b):
    return mm(a[0], b[0]) + (mm(a[0], b[1]) + mm(a[1], b[0]))


def product(a, b):
    return dot3(split(a), split(b))


def place():
    vec = lax.axis_index("vec")
    return lax.shift_right_logical(vec, 2), vec & 3, lax.axis_index("row") & 1


def assemble(parts, buf, start=0):
    far, near, _ = place()
    width = buf.shape[2]
    for step, part in zip((0, 1, 3, 2), parts):
        x = near ^ step
        for z in range(2):
            buf[(far ^ z) * XS + x] = part[16 * z : 16 * z + 16, start : start + width]


def block(buf, start, width):
    return buf[:, :, start : start + width].reshape(NB, width)


def group_matrix(basis_t, factor):
    return product(basis_t.T, product(factor, basis_t))


def put(refs, index, value):
    high, low = split(value)
    refs[0][index] = high
    refs[1][index] = low


def get(refs, *index):
    return refs[0][index], refs[1][index]


def look_ahead(side, nxt_t, matrix):
    zero = jnp.zeros((NB, NB), F32)
    if side == 0:
        return jnp.concatenate([nxt_t, zero], axis=1) - product(nxt_t, matrix[:NB])
    return jnp.concatenate([zero, nxt_t], axis=1) - product(nxt_t, matrix[NB:])


def spans(body, width):
    def step(c, carry):
        body(pl.ds(pl.multiple_of(c * SPAN, SPAN), SPAN))
        return carry

    lax.fori_loop(0, width // SPAN, step, 0)


def lay(out, *parts):
    at = 0
    for part in parts:
        out[:, at : at + part.shape[1]] = part
        at += part.shape[1]


def ends(turned, r):
    return turned[r, :, 0:128], turned[r, :, 384:512]


def shift_kernel(factors, shifted):
    lay(shifted, *(factors[r, g] for r, g in SHIFTED))


def first_payload_kernel(turned, factors, out):
    lay(
        out,
        turned[0], *ends(turned, 1), factors[0, 0], factors[0, 1],
        turned[1, :, 128:384], factors[1, 0], factors[1, 1],
    )


def rest_payload_kernel(turned, factors, slid, out):
    came = [slid[:, k * NB : (k + 1) * NB] for k in range(8)]
    lay(
        out,
        came[0], came[1], factors[2, 0], *ends(turned, 3),
        turned[3, :, 128:384], came[3], factors[3, 0], came[2], turned[4], came[4], came[5], *ends(turned, 5),
        turned[5, :, 128:384], came[6], came[7], turned[2],
    )


def first_kernel(own, left, right, across, x, ph, pl_, chip, core, nxt_t, buf, lh, ll):
    assemble((own, left, right, across), buf)
    odd = place()[2] == 1
    for side in range(2):
        nxt = block(buf, 512 + side * NB, NB)
        nxt_t[side] = nxt
        matrix = group_matrix(block(buf, side * 256, 256), block(buf, 768 + side * NB, NB))
        put((ph, pl_), side, matrix)
        put((lh, ll), side, look_ahead(side, nxt, matrix))

    def body(cols):
        heads = [
            dot3(get((lh, ll), side), split(x[side * 256 : side * 256 + 256, cols])) for side in range(2)
        ]
        chip[:, cols] = jnp.where(odd, heads[1], heads[0])
        core[:, cols] = jnp.where(odd, heads[0], heads[1])

    spans(body, x.shape[1])


def fill_kernel(own, left, right, across, nxt_t, ph, pl_, x, u, tail, buf, mh, ml):
    assemble((own, left, right, across), buf, 1024)
    put((mh, ml), slice(None), group_matrix(block(buf, 0, 256), block(buf, 256, NB)))
    tail[...] = product(nxt_t[1].T, block(buf, 384, NB))

    def body(cols):
        panels = []
        for side in range(2):
            panel = x[side * 256 : side * 256 + 256, cols]
            panels.append(panel - dot3((ph[side], pl_[side]), split(panel)))
        u[0:128, cols] = panels[0][:NB]
        u[384:512, cols] = panels[1][NB:]
        panel = jnp.concatenate([panels[0][NB:], panels[1][:NB]], axis=0)
        u[128:384, cols] = panel - dot3((mh[...], ml[...]), split(panel))

    spans(body, u.shape[1])


def packed(value):
    return jnp.concatenate([value[16 * k : 16 * k + 16] for k in range(8)], axis=1)


def unpacked(value):
    return jnp.concatenate([value[:, k * NB : (k + 1) * NB] for k in range(8)], axis=0)


def chosen(odd, values):
    return jnp.where(odd, values[1], values[0]), jnp.where(odd, values[0], values[1])


def spread_and_ahead(basis, buf, at, nxt_t, spread, chip, core, core_at, ph, pl_, uh, ul, lh, ll):
    tops = []
    for side in range(2):
        put((uh, ul), side, spread[side])
        nxt = block(buf, at + 256 + side * NB, NB)
        nxt_t[side] = nxt
        matrix = group_matrix(block(basis, side * 256, 256), block(buf, at + side * NB, NB))
        put((ph, pl_), side, matrix)
        look = look_ahead(side, nxt, matrix)
        put((lh, ll), side, look)
        tops.append(packed(product(look[:, :NB] if side == 0 else look[:, NB:], spread[side])))
    first, second = chosen(place()[2] == 1, tops)
    chip[NB : NB + 16, :] = first
    core[core_at + NB : core_at + NB + 16, :] = second


def ahead_kernel(prev_t, prev_tail, u, own, left, right, across, *rest):
    ph, pl_, uh, ul, chip, core, nxt_t, basis, buf, last_block, lh, ll = rest
    parts = (own, left, right, across)
    assemble(parts, basis, 2816)
    assemble(parts, buf)
    assemble(parts, last_block, 2816 - NB)
    odd = place()[2] == 1
    for k in range(8):
        chip[NB + 16 :, k * NB : (k + 1) * NB] = last_block[k]
        core[NB + 16 :, k * NB : (k + 1) * NB] = last_block[k]
    spread = (product(prev_t[0].T, block(buf, 0, NB)), prev_tail[...])
    spread_and_ahead(basis, buf, NB, nxt_t, spread, chip, core, 0, ph, pl_, uh, ul, lh, ll)

    def body(cols):
        heads = [dot3(get((lh, ll), side), split(u[side * 256 : side * 256 + 256, cols])) for side in range(2)]
        chip[:NB, cols], core[:NB, cols] = chosen(odd, heads)

    spans(body, u.shape[1])


def middle_kernel(own, left, right, across, prev_t, u_in, prev_core, *rest):
    u, ph, pl_, uh, ul, chip, core, nxt_t, buf, basis, tips, mh, ml, lh, ll = rest
    parts = (own, left, right, across)
    assemble(parts, buf, 640)
    assemble(parts, basis, 1280)
    assemble(parts, tips, 1792)
    odd = place()[2] == 1
    start = prev_core.shape[0]
    put((mh, ml), slice(None), group_matrix(block(buf, 0, 256), block(buf, 256, NB)))
    spread = (product(prev_t[0].T, block(buf, 512, NB)), product(prev_t[1].T, block(buf, 384, NB)))
    spread_and_ahead(basis, tips, 0, nxt_t, spread, chip, core, start, ph, pl_, uh, ul, lh, ll)

    def body(cols):
        core[:start, cols] = prev_core[:, cols]
        panel = u_in[128:384, cols]
        panel = panel - dot3((mh[...], ml[...]), split(panel))
        u[128:384, cols] = panel
        top, bottom = u_in[0:128, cols], u_in[384:512, cols]
        u[0:128, cols] = top
        u[384:512, cols] = bottom
        heads = [
            dot3(get((lh, ll), 0), split(jnp.concatenate([top, panel[:NB]], axis=0))),
            dot3(get((lh, ll), 1), split(jnp.concatenate([panel[NB:], bottom], axis=0))),
        ]
        chip[:NB, cols], core[start : start + NB, cols] = chosen(odd, heads)

    spans(body, u.shape[1])


def both_sides(own_chip, got_chip, own_core, got_core, core_at, rows, cols):
    odd = place()[2] == 1
    lower = slice(core_at + rows.start, core_at + rows.stop)
    chip = own_chip[rows, cols] + got_chip[rows, cols]
    core = own_core[lower, cols] + got_core[lower, cols]
    return chosen(odd, (chip, core))


STRIP = slice(0, NB)
OPERATOR = slice(NB, NB + 16)
BLOCK = slice(NB + 16, NB + 32)
EVERY = slice(None)


def even_kernel(chip1, got1, core1, got_core1, uh, ul, ph, pl_, u_in, u):
    def body(cols):
        totals = both_sides(chip1, got1, core1, got_core1, 0, STRIP, cols)
        straddle_and_even(totals, uh, ul, ph, pl_, u_in, u, cols)

    spans(body, u.shape[1])


def straddle_and_even(totals, uh, ul, ph, pl_, u_in, u, cols):
    for side in range(2):
        near = slice(0, 128) if side == 0 else slice(384, 512)
        far = slice(128, 256) if side == 0 else slice(256, 384)
        panel = u_in[near, cols] - dot3((uh[side], ul[side]), split(totals[side]))
        pair = [panel, u_in[far, cols]] if side == 0 else [u_in[far, cols], panel]
        both = jnp.concatenate(pair, axis=0)
        u[side * 256 : side * 256 + 256, cols] = both - dot3((ph[side], pl_[side]), split(both))


def late_even_kernel(chip1, got1, core1, got_core1, chip3, got3, core35, got_core35, uh, ul, ph, pl_, u_in, *rest):
    u, sums, qh, ql = rest
    three = (chip3, got3, core35, got_core35)
    for side, value in enumerate(both_sides(*three, 0, OPERATOR, EVERY)):
        put((qh, ql), side, unpacked(value))

    def body(cols):
        ones = both_sides(chip1, got1, core1, got_core1, 0, STRIP, cols)
        threes = both_sides(*three, 0, STRIP, cols)
        totals = [threes[side] - dot3(get((qh, ql), side), split(ones[side])) for side in range(2)]
        for side in range(2):
            sums[side, :, cols] = totals[side]
        straddle_and_even(totals, uh, ul, ph, pl_, u_in, u, cols)

    spans(body, u.shape[1])


def final_middle_kernel(own, left, right, across, prev_t, u_in, got3, got_core35, *rest):
    out, uh, ul, buf, mh, ml, rows, sem = rest
    assemble((own, left, right, across), buf, 2304)
    put((mh, ml), slice(None), group_matrix(block(buf, 0, 256), block(buf, 256, NB)))
    copies = []
    for c in range(u_in.shape[1] // SPAN):
        cols = slice(c * SPAN, c * SPAN + SPAN)
        panel = u_in[128:384, cols]
        rows[c] = panel - dot3((mh[...], ml[...]), split(panel))
        copies.append(pltpu.make_async_copy(rows.at[c], out.at[128:384, cols], sem.at[c]))
        copies[-1].start()
    head = unpacked(jnp.where(place()[2] == 1, got_core35[BLOCK, :], got3[BLOCK, :]))
    put((uh, ul), 0, product(prev_t[0].T, head))
    put((uh, ul), 1, product(prev_t[1].T, block(buf, 384, NB)))
    for copy in copies:
        copy.wait()


def last_kernel(chip5, got5, core35, got_core35, sums, uh, ul, u_in, held_out, out, qh, ql, rows, sem):
    del held_out
    start = core35.shape[0] - chip5.shape[0]
    five = (chip5, got5, core35, got_core35)
    for side, value in enumerate(both_sides(*five, start, OPERATOR, EVERY)):
        put((qh, ql), side, unpacked(value))
    copies = []
    for c in range(u_in.shape[1] // SPAN):
        cols = slice(c * SPAN, c * SPAN + SPAN)
        fives = both_sides(*five, start, STRIP, cols)
        for side in range(2):
            near = slice(0, 128) if side == 0 else slice(384, 512)
            k = 2 * c + side
            total = fives[side] - dot3(get((qh, ql), side), split(sums[side, :, cols]))
            rows[k] = u_in[near, cols] - dot3((uh[side], ul[side]), split(total))
            copies.append(pltpu.make_async_copy(rows.at[k], out.at[near, cols], sem.at[k]))
            copies[-1].start()
    for copy in copies:
        copy.wait()


def call(kernel, outs, scratch, flops, *args, far=(), far_out=(), sems=0, aliases={}):
    vmem = pl.BlockSpec(memory_space=pltpu.VMEM)
    hbm = pl.BlockSpec(memory_space=pltpu.HBM)
    return pl.pallas_call(
        kernel,
        out_shape=[jax.ShapeDtypeStruct(s, t) for s, t in outs],
        in_specs=[hbm if k in far else vmem for k in range(len(args))],
        out_specs=[hbm if k in far_out else vmem for k in range(len(outs))],
        input_output_aliases=aliases,
        scratch_shapes=[pltpu.VMEM(s, t) for s, t in scratch] + [pltpu.SemaphoreType.DMA((sems,))] * bool(sems),
        cost_estimate=pl.CostEstimate(flops=flops, bytes_accessed=0 if far else 4 << 20, transcendentals=0),
        compiler_params=pltpu.CompilerParams(vmem_limit_bytes=24 << 20),
    )(*args)


def far_half(payload):
    return lax.ppermute(payload, "vec", [(v, v ^ XS) for v in range(2 * XS)])


def near_parts(payload, other):
    both = jnp.concatenate([payload, other], axis=0)
    parts = [lax.ppermute(both, "vec", [(v, v ^ step) for v in range(2 * XS)]) for step in (1, 3, 2)]
    return (both, *parts)


def rounds(eigvecs, reflectors, factors):
    rows = lax.axis_size("row")
    chip_pairs = [p for k in range(1, rows - 1, 2) for p in ((k, k + 1), (k + 1, k))]
    core_pairs = [(k, k ^ 1) for k in range(rows)]
    turned = jnp.transpose(reflectors, (0, 2, 1))
    (shifted,) = call(shift_kernel, [((16, 1024), F32)], [], 1 << 20, factors)
    slid = lax.ppermute(shifted, "row", [(k, k + 1) for k in range(rows - 1)])
    (a,) = call(first_payload_kernel, [((16, 1536), F32)], [], 1 << 20, turned, factors)
    a2 = far_half(a)
    (b,) = call(rest_payload_kernel, [((16, 3328), F32)], [], 1 << 20, turned, factors, slid)
    b2 = far_half(b)
    a = near_parts(a, a2)
    b = near_parts(b, b2)

    width = eigvecs.shape[1]
    whole = ((4 * NB, width), F32)
    strip = ((NB, width), F32)
    pair = ((2, 2 * NB, 2 * NB), BF16)
    small = ((2, NB, NB), BF16)
    ends_t = ((2, NB, NB), F32)
    strips = ((2, NB, width), F32)
    look = ((2, NB, 2 * NB), BF16)
    mid = ((2 * NB, 2 * NB), BF16)

    def held(lanes):
        return ((2 * XS, 16, lanes), F32)

    def across_chips(value):
        return lax.ppermute(value, "row", chip_pairs)

    def across_cores(value):
        return lax.ppermute(value, "row", core_pairs)

    unit = 2 * NB * NB * width * 3
    p0h, p0l, chip, core, nxt_t = call(
        first_kernel,
        [pair, pair, strip, strip, ends_t],
        [held(1024), look, look],
        4 * unit,
        *a, eigvecs,
    )
    ones = (chip, across_chips(chip), core, across_cores(core))
    u, tail = call(
        fill_kernel,
        [whole, ((NB, NB), F32)],
        [held(512), mid, mid],
        12 * unit,
        *a, nxt_t, p0h, p0l, eigvecs,
    )
    long = ((NB + 32, width), F32)
    shorter = ((NB + 16, width), F32)
    double = ((2 * NB + 48, width), F32)
    ph, pl_, uh, ul, chip3, core3, nxt_t = call(
        ahead_kernel,
        [pair, pair, small, small, long, long, ends_t],
        [held(512), held(640), held(NB), look, look],
        4 * unit,
        nxt_t, tail, u, *b,
    )
    got3 = across_chips(chip3)
    (u,) = call(even_kernel, [whole], [], 10 * unit, *ones, uh, ul, ph, pl_, u)
    u, ph, pl_, uh, ul, chip5, core35, nxt_t = call(
        middle_kernel,
        [whole, pair, pair, small, small, shorter, double, ends_t],
        [held(640), held(512), held(512), mid, mid, look, look],
        10 * unit,
        *b, nxt_t, u, core3,
    )
    got5 = across_chips(chip5)
    got_core35 = across_cores(core35)
    u, sums = call(
        late_even_kernel,
        [whole, strips],
        [small, small],
        12 * unit,
        *ones, chip3, got3, core35, got_core35, uh, ul, ph, pl_, u,
    )
    out, uh, ul = call(
        final_middle_kernel,
        [whole, small, small],
        [held(512), mid, mid, ((width // SPAN, 2 * NB, SPAN), F32)],
        5 * unit,
        *b, nxt_t, u, got3, got_core35,
        far_out=(0,),
        sems=width // SPAN,
    )
    (out,) = call(
        last_kernel,
        [whole],
        [small, small, ((2 * width // SPAN, NB, SPAN), F32)],
        4 * unit,
        chip5, got5, core35, got_core35, sums, uh, ul, u, out,
        far=(8,),
        far_out=(0,),
        sems=2 * width // SPAN,
        aliases={8: 0},
    )
    return out


def solution(mesh):
    return jax.shard_map(
        rounds,
        mesh=mesh,
        in_specs=(P("row", "vec"), P(None, "row", "vec"), P(None, "row", "vec", None)),
        out_specs=P("row", "vec"),
        check_vma=False,
    )
```

```python
import jax
import jax.numpy as jnp
from jax import lax
from jax.experimental import pallas as pl
from jax.experimental.pallas import tpu as pltpu
from jax.sharding import PartitionSpec as P


NB = 128
F32 = jnp.float32
BF16 = jnp.bfloat16
SPAN = 512
WIDE = 1024
EARLY = 2
XS = 4
SHIFTED = ((1, 1), (2, 1), (3, 0), (3, 1), (4, 0), (4, 1), (5, 0), (5, 1))


def split(x):
    high = x.astype(BF16)
    return high, (x - high.astype(F32)).astype(BF16)


def mm(a, b):
    return jnp.dot(a, b, preferred_element_type=F32)


def dot3(a, b):
    return mm(jnp.concatenate([a[0], a[0], a[1]], axis=1), jnp.concatenate([b[0], b[1], b[0]], axis=0))


def product(a, b):
    return dot3(split(a), split(b))


def place():
    vec = lax.axis_index("vec")
    return lax.shift_right_logical(vec, 2), vec & 3, lax.axis_index("row") & 1


def assemble(parts, buf, start=0):
    far, near, _ = place()
    width = buf.shape[2]
    for step, part in zip((0, 1, 3, 2), parts):
        x = near ^ step
        for z in range(2):
            buf[(far ^ z) * XS + x] = part[16 * z : 16 * z + 16, start : start + width]


def block(buf, start, width):
    return buf[:, :, start : start + width].reshape(NB, width)


def group_matrix(basis_t, factor):
    return product(basis_t.T, product(factor, basis_t))


def put(refs, index, value):
    high, low = split(value)
    refs[0][index] = high
    refs[1][index] = low


def get(refs, *index):
    return refs[0][index], refs[1][index]


def look_ahead(side, nxt_t, matrix):
    zero = jnp.zeros((NB, NB), F32)
    if side == 0:
        return jnp.concatenate([nxt_t, zero], axis=1) - product(nxt_t, matrix[:NB])
    return jnp.concatenate([zero, nxt_t], axis=1) - product(nxt_t, matrix[NB:])


def spans(body, width):
    for start in range(0, width, WIDE):
        body(slice(start, start + WIDE))


def lay(out, *parts):
    at = 0
    for part in parts:
        out[:, at : at + part.shape[1]] = part
        at += part.shape[1]


def halves(turned):
    return [turned[2, :, 0:256], turned[2, :, 256:512]]


def ends(turned, r):
    return turned[r, :, 0:128], turned[r, :, 384:512]


def shift_kernel(factors, shifted):
    lay(shifted, *(factors[r, g] for r, g in SHIFTED))


def first_payload_kernel(turned, factors, out):
    lay(
        out,
        turned[0], *ends(turned, 1), factors[0, 0], factors[0, 1],
        turned[1, :, 128:384], factors[1, 0], factors[1, 1], *halves(turned)[:EARLY],
    )


def rest_payload_kernel(turned, factors, slid, out):
    came = [slid[:, k * NB : (k + 1) * NB] for k in range(8)]
    lay(
        out,
        came[0], came[1], factors[2, 0], *ends(turned, 3),
        turned[3, :, 128:384], came[3], factors[3, 0], came[2], turned[4], came[4], came[5], *ends(turned, 5),
        turned[5, :, 128:384], came[6], came[7], *halves(turned)[EARLY:],
    )


def first_kernel(own, left, right, across, x, ph, pl_, chip, core, nxt_t, buf, lh, ll):
    assemble((own, left, right, across), buf)
    odd = place()[2] == 1
    for side in range(2):
        nxt = block(buf, 512 + side * NB, NB)
        nxt_t[side] = nxt
        matrix = group_matrix(block(buf, side * 256, 256), block(buf, 768 + side * NB, NB))
        put((ph, pl_), side, matrix)
        put((lh, ll), side, look_ahead(side, nxt, matrix))

    def body(cols):
        heads = [
            dot3(get((lh, ll), side), split(x[side * 256 : side * 256 + 256, cols])) for side in range(2)
        ]
        chip[:, cols] = jnp.where(odd, heads[1], heads[0])
        core[:, cols] = jnp.where(odd, heads[0], heads[1])

    spans(body, x.shape[1])


def fill_kernel(own, left, right, across, nxt_t, ph, pl_, x, u, tail, buf, mh, ml):
    assemble((own, left, right, across), buf, 1024)
    put((mh, ml), slice(None), group_matrix(block(buf, 0, 256), block(buf, 256, NB)))
    tail[...] = product(nxt_t[1].T, block(buf, 384, NB))

    def body(cols):
        panels = []
        for side in range(2):
            panel = x[side * 256 : side * 256 + 256, cols]
            panels.append(panel - dot3((ph[side], pl_[side]), split(panel)))
        u[0:128, cols] = panels[0][:NB]
        u[384:512, cols] = panels[1][NB:]
        panel = jnp.concatenate([panels[0][NB:], panels[1][:NB]], axis=0)
        u[128:384, cols] = panel - dot3((mh[...], ml[...]), split(panel))

    spans(body, u.shape[1])


def packed(value):
    return jnp.concatenate([value[16 * k : 16 * k + 16] for k in range(8)], axis=1)


def unpacked(value):
    return jnp.concatenate([value[:, k * NB : (k + 1) * NB] for k in range(8)], axis=0)


def chosen(odd, values):
    return jnp.where(odd, values[1], values[0]), jnp.where(odd, values[0], values[1])


def spread_and_ahead(bases, buf, at, nxt_t, spread, chip, core, core_at, ph, pl_, uh, ul, lh, ll):
    tops = []
    for side in range(2):
        put((uh, ul), side, spread[side])
        nxt = block(buf, at + 256 + side * NB, NB)
        nxt_t[side] = nxt
        matrix = group_matrix(bases[side], block(buf, at + side * NB, NB))
        put((ph, pl_), side, matrix)
        look = look_ahead(side, nxt, matrix)
        put((lh, ll), side, look)
        tops.append(packed(product(look[:, :NB] if side == 0 else look[:, NB:], spread[side])))
    first, second = chosen(place()[2] == 1, tops)
    chip[NB : NB + 16, :] = first
    core[core_at + NB : core_at + NB + 16, :] = second


def ahead_kernel(prev_t, prev_tail, u, *rest):
    early, parts = rest[:4], rest[4:8]
    ph, pl_, uh, ul, chip, core, nxt_t, first_basis, second_basis, buf, last_block, lh, ll = rest[8:]
    bases = (first_basis, second_basis)
    for side, basis in enumerate(bases):
        if side < EARLY:
            assemble(early, basis, 1536 + 256 * side)
        else:
            assemble(parts, basis, 2816 + 256 * (side - EARLY))
    assemble(parts, buf)
    assemble(parts, last_block, 2816 - NB)
    odd = place()[2] == 1
    for k in range(8):
        chip[NB + 16 :, k * NB : (k + 1) * NB] = last_block[k]
        core[NB + 16 :, k * NB : (k + 1) * NB] = last_block[k]
    spread = (product(prev_t[0].T, block(buf, 0, NB)), prev_tail[...])
    spread_and_ahead([block(b, 0, 256) for b in bases], buf, NB, nxt_t, spread, chip, core, 0, ph, pl_, uh, ul, lh, ll)

    def body(cols):
        heads = [dot3(get((lh, ll), side), split(u[side * 256 : side * 256 + 256, cols])) for side in range(2)]
        chip[:NB, cols], core[:NB, cols] = chosen(odd, heads)

    spans(body, u.shape[1])


def middle_kernel(
    chip1, got1, core1, got_core1, uh1, ul1, ph2, pl2, own, left, right, across, prev_t, u_in, prev_core, *rest
):
    u, ph, pl_, uh, ul, chip, core, nxt_t, buf, basis, tips, mh, ml, lh, ll = rest
    parts = (own, left, right, across)
    assemble(parts, buf, 640)
    assemble(parts, basis, 1280)
    assemble(parts, tips, 1792)
    odd = place()[2] == 1
    start = prev_core.shape[0]
    put((mh, ml), slice(None), group_matrix(block(buf, 0, 256), block(buf, 256, NB)))
    spread = (product(prev_t[0].T, block(buf, 512, NB)), product(prev_t[1].T, block(buf, 384, NB)))
    spread_and_ahead([block(basis, 256 * k, 256) for k in range(2)], tips, 0, nxt_t, spread, chip, core, start, ph, pl_, uh, ul, lh, ll)

    def body(cols):
        core[:start, cols] = prev_core[:, cols]
        totals = both_sides(chip1, got1, core1, got_core1, 0, STRIP, cols)
        upper, lower = straddle_and_even(totals, uh1, ul1, ph2, pl2, u_in, cols)
        panel = jnp.concatenate([upper[NB:], lower[:NB]], axis=0)
        panel = panel - dot3((mh[...], ml[...]), split(panel))
        top, bottom = upper[:NB], lower[NB:]
        u[128:384, cols] = panel
        u[0:128, cols] = top
        u[384:512, cols] = bottom
        heads = [
            dot3(get((lh, ll), 0), split(jnp.concatenate([top, panel[:NB]], axis=0))),
            dot3(get((lh, ll), 1), split(jnp.concatenate([panel[NB:], bottom], axis=0))),
        ]
        chip[:NB, cols], core[start : start + NB, cols] = chosen(odd, heads)

    spans(body, u.shape[1])


def both_sides(own_chip, got_chip, own_core, got_core, core_at, rows, cols):
    odd = place()[2] == 1
    lower = slice(core_at + rows.start, core_at + rows.stop)
    chip = own_chip[rows, cols] + got_chip[rows, cols]
    core = own_core[lower, cols] + got_core[lower, cols]
    return chosen(odd, (chip, core))


STRIP = slice(0, NB)
OPERATOR = slice(NB, NB + 16)
BLOCK = slice(NB + 16, NB + 32)
EVERY = slice(None)


def straddle_and_even(totals, uh, ul, ph, pl_, u_in, cols):
    halves = []
    for side in range(2):
        near = slice(0, 128) if side == 0 else slice(384, 512)
        far = slice(128, 256) if side == 0 else slice(256, 384)
        panel = u_in[near, cols] - dot3((uh[side], ul[side]), split(totals[side]))
        pair = [panel, u_in[far, cols]] if side == 0 else [u_in[far, cols], panel]
        both = jnp.concatenate(pair, axis=0)
        halves.append(both - dot3((ph[side], pl_[side]), split(both)))
    return halves


def operators_kernel(own, left, right, across, prev_t, mh, ml, uh, ul, buf):
    assemble((own, left, right, across), buf, 2304)
    put((mh, ml), slice(None), group_matrix(block(buf, 0, 256), block(buf, 256, NB)))
    put((uh, ul), slice(None), product(prev_t[1].T, block(buf, 384, NB)))


def final_middle_kernel(
    chip1, got1, core1, got_core1, chip3, got3, core35, got_core35, uh3, ul3, ph, pl_, mh, ml, th, tl, prev_t, u_in, *rest
):
    strips, center, sums, uh, ul, qh, ql = rest
    three = (chip3, got3, core35, got_core35)
    for side, value in enumerate(both_sides(*three, 0, OPERATOR, EVERY)):
        put((qh, ql), side, unpacked(value))

    def body(cols):
        ones = both_sides(chip1, got1, core1, got_core1, 0, STRIP, cols)
        threes = both_sides(*three, 0, STRIP, cols)
        totals = [threes[side] - dot3(get((qh, ql), side), split(ones[side])) for side in range(2)]
        for side in range(2):
            sums[side, :, cols] = totals[side]
        upper, lower = straddle_and_even(totals, uh3, ul3, ph, pl_, u_in, cols)
        strips[0, :, cols] = upper[:NB]
        strips[1, :, cols] = lower[NB:]
        panel = jnp.concatenate([upper[NB:], lower[:NB]], axis=0)
        center[:, cols] = panel - dot3((mh[...], ml[...]), split(panel))

    spans(body, u_in.shape[1])
    head = unpacked(jnp.where(place()[2] == 1, got_core35[BLOCK, :], got3[BLOCK, :]))
    put((uh, ul), 0, product(prev_t[0].T, head))
    uh[1] = th[...]
    ul[1] = tl[...]


def last_kernel(chip5, got5, core35, got_core35, sums, uh, ul, strips, center, out, qh, ql, rows, sem):
    count = 2 * sums.shape[2] // SPAN
    copies = [pltpu.make_async_copy(center, out.at[128:384, :], sem.at[count])]
    copies[0].start()
    start = core35.shape[0] - chip5.shape[0]
    five = (chip5, got5, core35, got_core35)
    for side, value in enumerate(both_sides(*five, start, OPERATOR, EVERY)):
        put((qh, ql), side, unpacked(value))
    for c in range(sums.shape[2] // SPAN):
        cols = slice(c * SPAN, c * SPAN + SPAN)
        fives = both_sides(*five, start, STRIP, cols)
        for side in range(2):
            near = slice(0, 128) if side == 0 else slice(384, 512)
            k = 2 * c + side
            total = fives[side] - dot3(get((qh, ql), side), split(sums[side, :, cols]))
            rows[k] = strips[side, :, cols] - dot3((uh[side], ul[side]), split(total))
            copies.append(pltpu.make_async_copy(rows.at[k], out.at[near, cols], sem.at[k]))
            copies[-1].start()
    for copy in copies:
        copy.wait()


def call(kernel, outs, scratch, flops, *args, far=(), far_out=(), sems=0):
    vmem = pl.BlockSpec(memory_space=pltpu.VMEM)
    hbm = pl.BlockSpec(memory_space=pltpu.HBM)
    return pl.pallas_call(
        kernel,
        out_shape=[jax.ShapeDtypeStruct(s, t) for s, t in outs],
        in_specs=[hbm if k in far else vmem for k in range(len(args))],
        out_specs=[hbm if k in far_out else vmem for k in range(len(outs))],
        scratch_shapes=[pltpu.VMEM(s, t) for s, t in scratch] + [pltpu.SemaphoreType.DMA((sems,))] * bool(sems),
        cost_estimate=pl.CostEstimate(flops=flops, bytes_accessed=0 if far else 4 << 20, transcendentals=0),
        compiler_params=pltpu.CompilerParams(vmem_limit_bytes=24 << 20),
    )(*args)


def far_half(payload):
    return lax.ppermute(payload, "vec", [(v, v ^ XS) for v in range(2 * XS)])


def near_parts(payload, other):
    both = jnp.concatenate([payload, other], axis=0)
    parts = [lax.ppermute(both, "vec", [(v, v ^ step) for v in range(2 * XS)]) for step in (1, 3, 2)]
    return (both, *parts)


def rounds(eigvecs, reflectors, factors):
    rows = lax.axis_size("row")
    chip_pairs = [p for k in range(1, rows - 1, 2) for p in ((k, k + 1), (k + 1, k))]
    core_pairs = [(k, k ^ 1) for k in range(rows)]
    turned = jnp.transpose(reflectors, (0, 2, 1))
    (shifted,) = call(shift_kernel, [((16, 1024), F32)], [], 1 << 20, factors)
    slid = lax.ppermute(shifted, "row", [(k, k + 1) for k in range(rows - 1)])
    (a,) = call(first_payload_kernel, [((16, 1536 + 256 * EARLY), F32)], [], 1 << 20, turned, factors)
    a2 = far_half(a)
    (b,) = call(rest_payload_kernel, [((16, 3328 - 256 * EARLY), F32)], [], 1 << 20, turned, factors, slid)
    b2 = far_half(b)
    a = near_parts(a, a2)
    b = near_parts(b, b2)

    width = eigvecs.shape[1]
    whole = ((4 * NB, width), F32)
    strip = ((NB, width), F32)
    pair = ((2, 2 * NB, 2 * NB), BF16)
    small = ((2, NB, NB), BF16)
    ends_t = ((2, NB, NB), F32)
    strips = ((2, NB, width), F32)
    look = ((2, NB, 2 * NB), BF16)
    mid = ((2 * NB, 2 * NB), BF16)

    def held(lanes):
        return ((2 * XS, 16, lanes), F32)

    def across_chips(value):
        return lax.ppermute(value, "row", chip_pairs)

    def across_cores(value):
        return lax.ppermute(value, "row", core_pairs)

    unit = 2 * NB * NB * width * 3
    p0h, p0l, chip, core, nxt_t = call(
        first_kernel,
        [pair, pair, strip, strip, ends_t],
        [held(1024), look, look],
        4 * unit,
        *a, eigvecs,
    )
    ones = (chip, across_chips(chip), core, across_cores(core))
    u, tail = call(
        fill_kernel,
        [whole, ((NB, NB), F32)],
        [held(512), mid, mid],
        12 * unit,
        *a, nxt_t, p0h, p0l, eigvecs,
    )
    long = ((NB + 32, width), F32)
    shorter = ((NB + 16, width), F32)
    double = ((2 * NB + 48, width), F32)
    ph, pl_, uh, ul, chip3, core3, nxt_t = call(
        ahead_kernel,
        [pair, pair, small, small, long, long, ends_t],
        [held(256), held(256), held(640), held(NB), look, look],
        4 * unit,
        nxt_t, tail, u, *a, *b,
    )
    got3 = across_chips(chip3)
    u, ph, pl_, uh, ul, chip5, core35, nxt_t = call(
        middle_kernel,
        [whole, pair, pair, small, small, shorter, double, ends_t],
        [held(640), held(512), held(512), mid, mid, look, look],
        20 * unit,
        *ones, uh, ul, ph, pl_, *b, nxt_t, u, core3,
    )
    got5 = across_chips(chip5)
    got_core35 = across_cores(core35)
    single = ((NB, NB), BF16)
    mh, ml, th, tl = call(operators_kernel, [mid, mid, single, single], [held(512)], unit, *b, nxt_t)
    tops, center, sums, uh, ul = call(
        final_middle_kernel,
        [strips, ((2 * NB, width), F32), strips, small, small],
        [small, small],
        20 * unit,
        *ones, chip3, got3, core35, got_core35, uh, ul, ph, pl_, mh, ml, th, tl, nxt_t, u,
    )
    (vectors,) = call(
        last_kernel,
        [whole],
        [small, small, ((2 * width // SPAN, NB, SPAN), F32)],
        4 * unit,
        chip5, got5, core35, got_core35, sums, uh, ul, tops, center,
        far_out=(0,),
        sems=2 * width // SPAN + 1,
    )
    return vectors


def solution(mesh):
    return jax.shard_map(
        rounds,
        mesh=mesh,
        in_specs=(P("row", "vec"), P(None, "row", "vec"), P(None, "row", "vec", None)),
        out_specs=P("row", "vec"),
        check_vma=False,
    )
```
